512 devices in a mesh: row: 32 (over z, x_lo), col: 16 (over y, x_hi, core).
Axes of the slice: x: 4 (x_hi: 2, x_lo: 2; x = x_hi * 2 + x_lo), y: 4, z: 16, core: 2. Of those that a mesh axis runs over, the one named last changes fastest.
Arguments:
- grad: bfloat16 [262144, 1024], P(('row', 'col')), may hold values from -2500 to 2500
- left_root: bfloat16 [262144, 1024], P(('row', 'col')), may hold values from -0.051 to 3, as said below
- right_root: bfloat16 [262144, 1024], P(('row', 'col')), may hold values from -0.051 to 3, as said below
Outputs:
- update: bfloat16 [262144, 1024], P(('row', 'col'))
The draws below stay inside these ranges and needn't reach their ends.
Inputs may be any that keep to these rules, and one draw needn't show every extreme that they name: `left_root`: each block L_b is symmetric and positive definite. `right_root`: each block R_b is symmetric and positive definite.
All inputs are finite; a program needn't handle non-finite values.
Results may differ from the reference program's by a relative error of at most 0.0049.
Values may be sent and summed in bfloat16 or wider, within the bound.
No kernel may reach another device: no remote copies, remote signals or barrier semaphores. Data moves between devices by JAX's collectives and lax.ppermute only.
A program may use at most 64 MiB of HBM per device.

```python
import math
import jax
import jax.numpy as jnp
from jax import lax

BLK = 1024
NB = 256


def root_blocks(key, stream):
    folded = jax.random.fold_in(key, stream)
    k_diagonal, k_entries = jax.random.split(folded)
    diagonal = jnp.exp(jax.random.uniform(k_diagonal, (NB, BLK), jnp.float32, math.log(0.6), math.log(2.0)))
    entries = jnp.clip(jax.random.normal(k_entries, (NB, BLK, BLK), jnp.float32), -4.0, 4.0)
    spread = 0.26
    symmetric = (entries + jnp.swapaxes(entries, 1, 2)) * (spread / math.sqrt(2.0 * BLK))
    symmetric = jnp.clip(symmetric, -0.05, 0.05)
    identity = jnp.eye(BLK, dtype=jnp.float32)
    blocks = symmetric * (1.0 - identity) + diagonal[:, :, None] * identity
    return blocks.reshape(NB * BLK, BLK).astype(jnp.bfloat16)


def draw_left_root(key, part):
    return root_blocks(key, 11)


def draw_right_root(key, part):
    return root_blocks(key, 23)


def draw_grad(key, part):
    k_noise, k_rows, k_cols = jax.random.split(jax.random.fold_in(key, 5), 3)
    position = jnp.arange(NB, dtype=jnp.float32) / max(NB - 1, 1)
    gaussian = jnp.clip(jax.random.normal(k_noise, (NB, BLK, BLK), jnp.float32), -6.0, 6.0)
    row_scale = jnp.exp(jax.random.uniform(k_rows, (NB, BLK), jnp.float32, 0.0, math.log(10.0)))
    col_scale = jnp.exp(jax.random.uniform(k_cols, (NB, BLK), jnp.float32, 0.0, math.log(10.0)))
    block_scale = jnp.sqrt(1.0 + 2.0 * position)
    values = gaussian * row_scale[:, :, None] * col_scale[:, None, :] * block_scale[:, None, None]
    return values.reshape(NB * BLK, BLK).astype(jnp.bfloat16)


def setup_inputs(seed: int = 0) -> dict:
    key_list = jax.random.split(jax.random.key(seed), 4)
    return {
        "grad": draw_grad(jax.random.fold_in(key_list[3], 71), 0),
        "left_root": draw_left_root(jax.random.fold_in(key_list[3], 71), 0),
        "right_root": draw_right_root(jax.random.fold_in(key_list[3], 71), 0),
    }


epsilon = 1e-06
clip_rms = 1.0

def reference(grad, left_root, right_root):
    grad_blocks = grad.reshape(NB, BLK, BLK)
    left_blocks = left_root.reshape(NB, BLK, BLK)
    right_blocks = right_root.reshape(NB, BLK, BLK)
    global_sq = jnp.sum(jnp.square(grad.astype(jnp.float32)))
    entries_all = NB * BLK * BLK
    clip_factor = clip_rms / jnp.sqrt(global_sq / entries_all + epsilon)

    def one_block(operands):
        gradient, left_block, right_block = operands
        product = jnp.dot(gradient, right_block, preferred_element_type=jnp.float32).astype(jnp.bfloat16)
        precond = jnp.dot(left_block, product, preferred_element_type=jnp.float32)
        grad_sq = jnp.sum(jnp.square(gradient.astype(jnp.float32)))
        cond_sq = jnp.sum(precond * precond)
        graft_ratio = jnp.sqrt((grad_sq / (BLK * BLK) + epsilon) / (cond_sq / (BLK * BLK) + epsilon))
        return (clip_factor * graft_ratio * precond).astype(jnp.bfloat16)
    update = lax.map(one_block, (grad_blocks, left_blocks, right_blocks))
    return update.reshape(NB * BLK, BLK)
```

```python
import functools

import jax
import jax.numpy as jnp
from jax import lax
from jax.sharding import Mesh
from jax.sharding import PartitionSpec as P

BLK = 1024
COL = ("col_0", "col_1", "col_2")
ROW_COL = ("row_0", "row_1", "col_0", "col_1", "col_2")
ROW = ("row_0", "row_1")
PLANE = ("row_1", "col_0", "col_1", "col_2")
LINE = "row_0"


epsilon = 1e-06
clip_rms = 1.0


def partner(shard, axis, distance):
    return lax.ppermute(shard, axis, [(i, i ^ 1 << distance) for i in range(lax.axis_size(axis))])


def over_group(value, axes):
    members = lax.axis_size(axes)
    sent = jnp.full((members, 128), value)
    heard = lax.all_to_all(sent, axes, 0, 0, tiled=True)
    return jnp.sum(heard[:, 0])


def over_axes(shard, groups):
    return functools.reduce(over_group, groups, shard)


def apply_right(gradient_rows, own_start, other_start, rows_here, right_root, partner_right):
    own_cols = lax.dynamic_slice_in_dim(gradient_rows, own_start, rows_here, 1)
    other_cols = lax.dynamic_slice_in_dim(gradient_rows, other_start, rows_here, 1)
    applied = jnp.dot(own_cols, right_root, preferred_element_type=jnp.float32)
    applied = applied + jnp.dot(other_cols, partner_right, preferred_element_type=jnp.float32)
    return applied.astype(jnp.bfloat16)


def shards(grad, left_root, right_root):
    rows_here = grad.shape[0]
    parity = lax.axis_index(COL) % 2
    own_start = parity * rows_here
    other_start = (1 - parity) * rows_here
    partner_right = partner(right_root, COL, 0)
    right_applied = apply_right(grad, own_start, other_start, rows_here, right_root, partner_right)
    partner_rows = partner(right_applied, COL, 0)
    own_left = lax.dynamic_slice_in_dim(left_root, own_start, rows_here, 1)
    other_left = lax.dynamic_slice_in_dim(left_root, other_start, rows_here, 1)
    preconditioned = jnp.dot(own_left, right_applied, preferred_element_type=jnp.float32)
    preconditioned = preconditioned + jnp.dot(
        other_left, partner_rows, preferred_element_type=jnp.float32
    )
    grad_sq = jnp.sum(jnp.square(grad.astype(jnp.float32)))
    cond_sq = jnp.sum(preconditioned * preconditioned)
    global_sq = over_axes(grad_sq, (PLANE, LINE))
    partner_sums = partner(jnp.stack([grad_sq, cond_sq]), COL, 0)
    block_grad = grad_sq + partner_sums[0]
    block_cond = cond_sq + partner_sums[1]
    block_count = BLK * BLK
    total_count = lax.axis_size(ROW) * lax.axis_size(COL) // 2 * block_count
    clip_factor = clip_rms / jnp.sqrt(global_sq / total_count + epsilon)
    graft_ratio = jnp.sqrt(
        (block_grad / block_count + epsilon) / (block_cond / block_count + epsilon)
    )
    return (clip_factor * graft_ratio * preconditioned).astype(jnp.bfloat16)


def solution(mesh):
    torus = Mesh(
        mesh.devices.reshape(16, 2, 4, 2, 2), ("row_0", "row_1", "col_0", "col_1", "col_2")
    )
    return jax.shard_map(
        shards,
        mesh=torus,
        in_specs=(P(ROW_COL, None), P(ROW_COL, None), P(ROW_COL, None)),
        out_specs=P(ROW_COL, None),
        check_vma=False,
    )
```

```python
import functools

import jax
import jax.numpy as jnp
from jax import lax
from jax.experimental import pallas as pl
from jax.experimental.pallas import tpu as pltpu
from jax.sharding import Mesh
from jax.sharding import PartitionSpec as P

BLK = 1024
PLANE = ("row_1", "col_0", "col_1", "col_2")
LINE = "row_0"
PAIR = "col_2"
ALL = ("row_0", "row_1", "col_0", "col_1", "col_2")
EARLY_PLANES = 5
TILE = 256
LANES = 128

epsilon = 1e-06
clip_rms = 1.0
f32 = jnp.float32


def partner(shard, axis):
    return lax.ppermute(shard, axis, [(i, i ^ 1) for i in range(lax.axis_size(axis))])


def in_hbm(array):
    return pltpu.with_memory_space_constraint(array, pltpu.HBM)


def in_vmem(array):
    return pltpu.with_memory_space_constraint(array, pltpu.VMEM)


def squares(values):
    values = values.astype(f32)
    rows, columns = values.shape
    return jnp.sum((values * values).reshape(rows // 8, 8, columns), axis=0)


def lane_sums(partial):
    rows = jnp.sum(partial, axis=0, keepdims=True)
    return sum(rows[:, i : i + LANES] for i in range(0, rows.shape[1], LANES))


def head_kernel(grad, left, right, held, sent, sems):
    rows = grad.shape[0]
    step = rows // 4
    pieces = []
    for i in range(4):
        piece = pl.ds(i * step, step)
        pieces.append(
            pltpu.make_async_copy(grad.at[piece], held.at[0, piece], sems.at[i])
        )
    others = [
        pltpu.make_async_copy(right, held.at[1], sems.at[4]),
        pltpu.make_async_copy(left, held.at[2], sems.at[5]),
    ]
    for copy in pieces + others:
        copy.start()
    total = jnp.zeros((8, grad.shape[1]), f32)
    for i, copy in enumerate(pieces):
        copy.wait()
        total = total + squares(held[0, pl.ds(i * step, step), :])
    sent[...] = jnp.broadcast_to(lane_sums(total), sent.shape)
    for copy in others:
        copy.wait()


VMEM = pl.BlockSpec(memory_space=pltpu.VMEM)
HBM = pl.BlockSpec(memory_space=pltpu.HBM)


def head(grad, left, right, members):
    rows, columns = grad.shape
    return pl.pallas_call(
        head_kernel,
        out_shape=(
            pltpu.VMEM((3, rows, columns), grad.dtype),
            pltpu.VMEM((members, LANES), f32),
        ),
        in_specs=[HBM, HBM, HBM],
        out_specs=(VMEM, VMEM),
        scratch_shapes=[pltpu.SemaphoreType.DMA((6,))],
        cost_estimate=pl.CostEstimate(
            flops=2 * rows * columns, bytes_accessed=6 * rows * columns, transcendentals=0
        ),
        compiler_params=pltpu.CompilerParams(vmem_limit_bytes=16 << 20),
        name="head",
    )(grad, left, right)


def products(grad, left, right, heard, kept, ratio, own, theirs, applied, result, stats, sems):
    rows, columns = grad.shape
    tiles = columns // TILE
    sources = (grad, right, left)
    near_copies = [pltpu.make_async_copy(sources[i], own.at[i], sems.at[i]) for i in range(3)]
    far_copies = [pltpu.make_async_copy(heard.at[i], theirs.at[i], sems.at[3 + i]) for i in range(3)]
    for i in range(3):
        near_copies[i].start()
        far_copies[i].start()
    parity = lax.axis_index(PAIR)
    near = pl.ds(pl.multiple_of(parity * rows, rows), rows)
    far = pl.ds(pl.multiple_of((1 - parity) * rows, rows), rows)
    for i in range(2):
        near_copies[i].wait()
        far_copies[i].wait()

    def dot(a, b):
        return jnp.dot(a, b, preferred_element_type=f32)

    @pl.loop(0, tiles)
    def _(i):
        tile = pl.ds(pl.multiple_of(i * TILE, TILE), TILE)
        top, bottom = own[1, :, tile], theirs[1, :, tile]
        mine = dot(own[0, :, near], top) + dot(own[0, :, far], bottom)
        applied[0, :, tile] = mine.astype(jnp.bfloat16)
        yours = dot(theirs[0, :, near], top) + dot(theirs[0, :, far], bottom)
        applied[1, :, tile] = yours.astype(jnp.bfloat16)

    near_copies[2].wait()
    far_copies[2].wait()

    def write(i):
        tile = pl.ds(pl.multiple_of(i * TILE, TILE), TILE)
        return pltpu.make_async_copy(result.at[:, tile], kept.at[:, tile], sems.at[6 + i])

    def second(i, cond_sq):
        tile = pl.ds(pl.multiple_of(i * TILE, TILE), TILE)
        top, bottom = applied[0, :, tile], applied[1, :, tile]
        mine = dot(own[2, :, near], top) + dot(own[2, :, far], bottom)
        result[:, tile] = mine
        yours = dot(theirs[2, :, near], top) + dot(theirs[2, :, far], bottom)
        return cond_sq + squares(mine) + squares(yours)

    cond_sq = lax.fori_loop(0, tiles, second, jnp.zeros((8, TILE), f32))
    for i in range(tiles):
        write(i).start()
    grad_sq = squares(own[0]) + squares(theirs[0])
    entries = BLK * BLK
    grad_sq = jnp.sum(lane_sums(grad_sq), axis=1, keepdims=True)
    cond_sq = jnp.sum(lane_sums(cond_sq), axis=1, keepdims=True)
    stats[...] = jnp.broadcast_to(
        jnp.sqrt((grad_sq / entries + epsilon) / (cond_sq / entries + epsilon)), stats.shape
    )
    copy = pltpu.make_async_copy(stats, ratio, sems.at[6 + tiles])
    copy.start()
    for i in range(tiles):
        write(i).wait()
    copy.wait()


def middle_kernel(plane, grad, left, right, heard, sent, kept, ratio, *scratch):
    sent[...] = jnp.broadcast_to(jnp.sum(plane[...], axis=0, keepdims=True), sent.shape)

    @pl.when(lax.axis_index(LINE) < EARLY_PLANES)
    def _():
        products(grad, left, right, heard, kept, ratio, *scratch)


def late_kernel(grad, left, right, heard, kept_in, ratio_in, kept, ratio, *scratch):
    @pl.when(lax.axis_index(LINE) >= EARLY_PLANES)
    def _():
        products(grad, left, right, heard, kept, ratio, *scratch)


def work_scratch(rows, columns):
    return [
        pltpu.VMEM((3, rows, columns), jnp.bfloat16),
        pltpu.VMEM((3, rows, columns), jnp.bfloat16),
        pltpu.VMEM((2, rows, columns), jnp.bfloat16),
        pltpu.VMEM((rows, columns), f32),
        pltpu.VMEM((8, LANES), f32),
        pltpu.SemaphoreType.DMA((7 + columns // TILE,)),
    ]


def middle(plane, grad, left, right, heard, members):
    rows, columns = grad.shape
    return pl.pallas_call(
        middle_kernel,
        out_shape=(
            jax.ShapeDtypeStruct((members, LANES), f32),
            pltpu.HBM((rows, columns), f32),
            pltpu.HBM((8, LANES), f32),
        ),
        in_specs=[VMEM, HBM, HBM, HBM, HBM],
        out_specs=(VMEM, HBM, HBM),
        scratch_shapes=work_scratch(rows, columns),
        cost_estimate=pl.CostEstimate(flops=10**9, bytes_accessed=10**7, transcendentals=0),
        compiler_params=pltpu.CompilerParams(vmem_limit_bytes=32 << 20),
        name="middle",
    )(plane, grad, left, right, heard)


def late(grad, left, right, heard, kept, ratio):
    rows, columns = grad.shape
    return pl.pallas_call(
        late_kernel,
        out_shape=(
            jax.ShapeDtypeStruct(kept.shape, f32),
            jax.ShapeDtypeStruct(ratio.shape, f32),
        ),
        in_specs=[HBM] * 6,
        out_specs=(HBM, HBM),
        input_output_aliases={4: 0, 5: 1},
        scratch_shapes=work_scratch(rows, columns),
        cost_estimate=pl.CostEstimate(flops=4 * 10**9, bytes_accessed=10**7, transcendentals=0),
        name="late",
    )(grad, left, right, heard, kept, ratio)


def final_kernel(count, line, kept, ratio, update, taken, staged, stats, sems):
    step = kept.shape[0] // 4
    pieces = [pl.ds(i * step, step) for i in range(4)]
    stat_copy = pltpu.make_async_copy(ratio, stats, sems.at[8])
    stat_copy.start()
    reads = [
        pltpu.make_async_copy(kept.at[piece], taken.at[piece], sems.at[i])
        for i, piece in enumerate(pieces)
    ]
    for copy in reads:
        copy.start()
    total = jnp.sum(jnp.sum(line[...], axis=0, keepdims=True), axis=1, keepdims=True)
    clip = clip_rms / jnp.sqrt(total / count + epsilon)
    stat_copy.wait()
    scale = clip * stats[0:1, 0:1]
    writes = []
    for i, piece in enumerate(pieces):
        reads[i].wait()
        staged[piece, :] = (scale * taken[piece, :]).astype(jnp.bfloat16)
        writes.append(pltpu.make_async_copy(staged.at[piece], update.at[piece], sems.at[4 + i]))
        writes[-1].start()
    for copy in writes:
        copy.wait()


def final(line, kept, ratio, count):
    rows, columns = kept.shape
    return pl.pallas_call(
        functools.partial(final_kernel, count),
        out_shape=jax.ShapeDtypeStruct((rows, columns), jnp.bfloat16),
        in_specs=[VMEM, HBM, HBM],
        out_specs=HBM,
        scratch_shapes=[
            pltpu.VMEM((rows, columns), f32),
            pltpu.VMEM((rows, columns), jnp.bfloat16),
            pltpu.VMEM((8, LANES), f32),
            pltpu.SemaphoreType.DMA((9,)),
        ],
        compiler_params=pltpu.CompilerParams(vmem_limit_bytes=16 << 20),
        name="final",
    )(line, kept, ratio)


def shards(grad, left_root, right_root):
    plane_size, line_size = lax.axis_size(PLANE), lax.axis_size(LINE)
    count = float(plane_size * line_size // 2 * BLK * BLK)
    grad, left_root, right_root = (in_hbm(x) for x in (grad, left_root, right_root))
    held, sent = head(grad, left_root, right_root, plane_size)
    with jax.named_scope("plane"):
        plane = lax.all_to_all(sent, PLANE, 0, 0, tiled=True)
    with jax.named_scope("exchange"):
        heard = in_hbm(partner(held, PAIR))
    sent, kept, ratio = middle(in_vmem(plane), grad, left_root, right_root, heard, line_size)
    with jax.named_scope("line"):
        line = lax.all_to_all(sent, LINE, 0, 0, tiled=True)
    kept, ratio = late(grad, left_root, right_root, heard, kept, ratio)
    return final(in_vmem(line), in_hbm(kept), in_hbm(ratio), count)


def solution(mesh):
    torus = Mesh(mesh.devices.reshape(16, 2, 4, 2, 2), ALL)
    return jax.shard_map(
        shards,
        mesh=torus,
        in_specs=(P(ALL, None), P(ALL, None), P(ALL, None)),
        out_specs=P(ALL, None),
        check_vma=False,
    )
```

```python
import functools

import jax
import jax.numpy as jnp
from jax import lax
from jax.experimental import pallas as pl
from jax.experimental.pallas import tpu as pltpu
from jax.sharding import Mesh
from jax.sharding import PartitionSpec as P

BLK = 1024
LINE, PLANE = "line", "plane"
ALL = (LINE, PLANE)
LINE_FIRST = 10
PLANE_FIRST = 30
EARLY_PLANES = 4
LANES = 128

epsilon = 1e-06
clip_rms = 1.0
f32 = jnp.float32


def partner(shard, axis):
    return lax.ppermute(shard, axis, [(i, i ^ 1) for i in range(lax.axis_size(axis))])


def tell_all(rows, axis, first):
    members = lax.axis_size(axis)
    group = [(first + i) % members for i in range(members)]
    return lax.all_to_all(rows, axis, 0, 0, axis_index_groups=[group], tiled=True)


def in_hbm(array):
    return pltpu.with_memory_space_constraint(array, pltpu.HBM)


def in_vmem(array):
    return pltpu.with_memory_space_constraint(array, pltpu.VMEM)


def squares(values):
    values = values.astype(f32)
    rows, columns = values.shape
    return jnp.sum((values * values).reshape(rows // 8, 8, columns), axis=0)


def lane_sums(partial):
    rows = jnp.sum(partial, axis=0, keepdims=True)
    return sum(rows[:, i : i + LANES] for i in range(0, rows.shape[1], LANES))


def head_kernel(grad, left, right, held, sent, sems):
    rows = grad.shape[0]
    step = rows // 4
    pieces = []
    for i in range(4):
        piece = pl.ds(i * step, step)
        pieces.append(
            pltpu.make_async_copy(grad.at[piece], held.at[0, piece], sems.at[i])
        )
    others = [
        pltpu.make_async_copy(right, held.at[1], sems.at[4]),
        pltpu.make_async_copy(left, held.at[2], sems.at[5]),
    ]
    for copy in pieces + others:
        copy.start()
    total = jnp.zeros((8, grad.shape[1]), f32)
    for i, copy in enumerate(pieces):
        copy.wait()
        total = total + squares(held[0, pl.ds(i * step, step), :])
    sent[...] = jnp.broadcast_to(lane_sums(total), sent.shape)
    for copy in others:
        copy.wait()


VMEM = pl.BlockSpec(memory_space=pltpu.VMEM)
HBM = pl.BlockSpec(memory_space=pltpu.HBM)
ANY = pl.BlockSpec(memory_space=pl.ANY)


def head(grad, left, right, members):
    rows, columns = grad.shape
    return pl.pallas_call(
        head_kernel,
        out_shape=(
            pltpu.VMEM((3, rows, columns), grad.dtype),
            pltpu.VMEM((members, LANES), f32),
        ),
        in_specs=[HBM, HBM, HBM],
        out_specs=(VMEM, VMEM),
        scratch_shapes=[pltpu.SemaphoreType.DMA((6,))],
        cost_estimate=pl.CostEstimate(
            flops=2 * rows * columns, bytes_accessed=6 * rows * columns, transcendentals=0
        ),
        compiler_params=pltpu.CompilerParams(vmem_limit_bytes=16 << 20),
        name="head",
    )(grad, left, right)


def products(own, held, ratio, applied, ready):
    rows = own.shape[1]
    parity = lax.axis_index(PLANE) % 2
    near = pl.ds(pl.multiple_of(parity * rows, rows), rows)
    far = pl.ds(pl.multiple_of((1 - parity) * rows, rows), rows)

    def both(left, top, bottom):
        first = jnp.dot(left[:, near], top[...], preferred_element_type=f32)
        return first + jnp.dot(left[:, far], bottom[...], preferred_element_type=f32)

    ready(1)
    applied[1] = both(held.at[0], own.at[1], held.at[1]).astype(jnp.bfloat16)
    grad_sq = squares(held[0])
    ready(0)
    applied[0] = both(own.at[0], own.at[1], held.at[1]).astype(jnp.bfloat16)
    grad_sq = grad_sq + squares(own[0])
    ready(2)
    result = both(own.at[2], applied.at[0], applied.at[1])
    upper = result.astype(jnp.bfloat16)
    held[0] = upper
    held[1] = (result - upper.astype(f32)).astype(jnp.bfloat16)
    cond_sq = squares(result) + squares(both(held.at[2], applied.at[0], applied.at[1]))
    entries = BLK * BLK
    grad_sq = jnp.sum(lane_sums(grad_sq), axis=1, keepdims=True)
    cond_sq = jnp.sum(lane_sums(cond_sq), axis=1, keepdims=True)
    ratio[...] = jnp.broadcast_to(
        jnp.sqrt((grad_sq / entries + epsilon) / (cond_sq / entries + epsilon)), ratio.shape
    )


def middle_kernel(plane, own, heard, sent, held, ratio, applied):
    sent[...] = jnp.broadcast_to(jnp.sum(plane[...], axis=0, keepdims=True), sent.shape)

    @pl.when(lax.axis_index(LINE) < EARLY_PLANES)
    def _():
        products(own, held, ratio, applied, lambda i: None)


def late_kernel(grad, right, left, heard, held, ratio, applied, own, sems):
    @pl.when(lax.axis_index(LINE) >= EARLY_PLANES)
    def _():
        copies = [
            pltpu.make_async_copy(source, own.at[i], sems.at[i])
            for i, source in enumerate((grad, right, left))
        ]
        for i in (1, 0, 2):
            copies[i].start()
        products(own, held, ratio, applied, lambda i: copies[i].wait())


def middle(plane, own, heard, members):
    _, rows, columns = heard.shape
    return pl.pallas_call(
        middle_kernel,
        out_shape=(
            pltpu.VMEM((members, LANES), f32),
            pltpu.VMEM(heard.shape, heard.dtype),
            pltpu.VMEM((8, LANES), f32),
        ),
        in_specs=[VMEM] * 3,
        out_specs=(VMEM,) * 3,
        input_output_aliases={2: 1},
        scratch_shapes=[pltpu.VMEM((2, rows, columns), jnp.bfloat16)],
        compiler_params=pltpu.CompilerParams(vmem_limit_bytes=24 << 20),
        cost_estimate=pl.CostEstimate(flops=10**9, bytes_accessed=10**7, transcendentals=0),
        name="middle",
    )(plane, own, heard)


def late(grad, right, left, heard):
    _, rows, columns = heard.shape
    return pl.pallas_call(
        late_kernel,
        out_shape=(pltpu.VMEM(heard.shape, heard.dtype), pltpu.VMEM((8, LANES), f32)),
        in_specs=[HBM, HBM, HBM, VMEM],
        out_specs=(VMEM, VMEM),
        input_output_aliases={3: 0},
        scratch_shapes=[
            pltpu.VMEM((2, rows, columns), jnp.bfloat16),
            pltpu.VMEM(heard.shape, heard.dtype),
            pltpu.SemaphoreType.DMA((3,)),
        ],
        compiler_params=pltpu.CompilerParams(vmem_limit_bytes=24 << 20),
        cost_estimate=pl.CostEstimate(flops=4 * 10**9, bytes_accessed=10**7, transcendentals=0),
        name="late",
    )(grad, right, left, heard)


def final_kernel(count, line, held, early_ratio, late_ratio, update, staged, sems):
    rows = held.shape[1]
    step = rows // 4
    total = jnp.sum(jnp.sum(line[...], axis=0, keepdims=True), axis=1, keepdims=True)
    clip = clip_rms / jnp.sqrt(total / count + epsilon)
    early = lax.axis_index(LINE) < EARLY_PLANES
    scale = clip * jnp.where(early, early_ratio[0:1, 0:1], late_ratio[0:1, 0:1])
    writes = []
    for i in range(4):
        piece = pl.ds(i * step, step)
        result = held[0, piece, :].astype(f32) + held[1, piece, :].astype(f32)
        staged[piece, :] = (scale * result).astype(jnp.bfloat16)
        writes.append(pltpu.make_async_copy(staged.at[piece], update.at[piece], sems.at[i]))
        writes[-1].start()
    for copy in writes:
        copy.wait()


def final(count, line, held, early_ratio, late_ratio):
    _, rows, columns = held.shape
    return pl.pallas_call(
        functools.partial(final_kernel, count),
        out_shape=jax.ShapeDtypeStruct((rows, columns), jnp.bfloat16),
        in_specs=[VMEM] * 4,
        out_specs=HBM,
        scratch_shapes=[
            pltpu.VMEM((rows, columns), jnp.bfloat16),
            pltpu.SemaphoreType.DMA((4,)),
        ],
        compiler_params=pltpu.CompilerParams(vmem_limit_bytes=16 << 20),
        name="final",
    )(line, held, early_ratio, late_ratio)


def shards(grad, left_root, right_root):
    plane_size, line_size = lax.axis_size(PLANE), lax.axis_size(LINE)
    count = float(plane_size * line_size // 2 * BLK * BLK)
    grad, left_root, right_root = (in_hbm(x) for x in (grad, left_root, right_root))
    own, sent = head(grad, left_root, right_root, plane_size)
    with jax.named_scope("plane"):
        plane = tell_all(sent, PLANE, PLANE_FIRST)
    with jax.named_scope("exchange"):
        heard = partner(own, PLANE)
    sent, held, early_ratio = middle(in_vmem(plane), own, heard, line_size)
    with jax.named_scope("line"):
        line = tell_all(sent, LINE, LINE_FIRST)
    held, late_ratio = late(grad, right_root, left_root, held)
    return final(count, in_vmem(line), held, early_ratio, late_ratio)


def solution(mesh):
    torus = Mesh(mesh.devices.reshape(16, 32), ALL)
    return jax.shard_map(
        shards,
        mesh=torus,
        in_specs=(P(ALL, None), P(ALL, None), P(ALL, None)),
        out_specs=P(ALL, None),
        check_vma=False,
    )
```

```python
import functools

import jax
import jax.numpy as jnp
from jax import lax
from jax.experimental import pallas as pl
from jax.experimental.pallas import tpu as pltpu
from jax.sharding import Mesh
from jax.sharding import PartitionSpec as P

BLK = 1024
LINE, PLANE = "line", "plane"
ALL = (LINE, PLANE)
LINE_FIRST = 10
PLANE_FIRST = 11
EARLY_PLANES = 4
LANES = 128

epsilon = 1e-06
clip_rms = 1.0
f32 = jnp.float32


def partner(shard, axis):
    return lax.ppermute(shard, axis, [(i, i ^ 1) for i in range(lax.axis_size(axis))])


def tell_all(rows, axis, first):
    members = lax.axis_size(axis)
    group = [(first + i) % members for i in range(members)]
    return lax.all_to_all(rows, axis, 0, 0, axis_index_groups=[group], tiled=True)


def in_hbm(array):
    return pltpu.with_memory_space_constraint(array, pltpu.HBM)


def in_vmem(array):
    return pltpu.with_memory_space_constraint(array, pltpu.VMEM)


def squares(values):
    values = values.astype(f32)
    rows, columns = values.shape
    return jnp.sum((values * values).reshape(rows // 8, 8, columns), axis=0)


def lane_sums(partial):
    rows = jnp.sum(partial, axis=0, keepdims=True)
    return sum(rows[:, i : i + LANES] for i in range(0, rows.shape[1], LANES))


def head_kernel(grad, left, right, held, sent, sems):
    rows = grad.shape[0]
    step = rows // 4
    pieces = []
    for i in range(4):
        piece = pl.ds(i * step, step)
        pieces.append(
            pltpu.make_async_copy(grad.at[piece], held.at[0, piece], sems.at[i])
        )
    others = [
        pltpu.make_async_copy(right, held.at[1], sems.at[4]),
        pltpu.make_async_copy(left, held.at[2], sems.at[5]),
    ]
    for copy in pieces + others:
        copy.start()
    total = jnp.zeros((8, grad.shape[1]), f32)
    for i, copy in enumerate(pieces):
        copy.wait()
        total = total + squares(held[0, pl.ds(i * step, step), :])
    sent[...] = jnp.broadcast_to(lane_sums(total), sent.shape)
    for copy in others:
        copy.wait()


VMEM = pl.BlockSpec(memory_space=pltpu.VMEM)
HBM = pl.BlockSpec(memory_space=pltpu.HBM)
ANY = pl.BlockSpec(memory_space=pl.ANY)


def head(grad, left, right, members):
    rows, columns = grad.shape
    return pl.pallas_call(
        head_kernel,
        out_shape=(
            pltpu.VMEM((3, rows, columns), grad.dtype),
            pltpu.VMEM((members, LANES), f32),
        ),
        in_specs=[HBM, HBM, HBM],
        out_specs=(VMEM, VMEM),
        scratch_shapes=[pltpu.SemaphoreType.DMA((6,))],
        cost_estimate=pl.CostEstimate(
            flops=2 * rows * columns, bytes_accessed=6 * rows * columns, transcendentals=0
        ),
        compiler_params=pltpu.CompilerParams(vmem_limit_bytes=16 << 20),
        name="head",
    )(grad, left, right)


def sides(rows):
    parity = lax.axis_index(PLANE) % 2
    near = pl.ds(pl.multiple_of(parity * rows, rows), rows)
    far = pl.ds(pl.multiple_of((1 - parity) * rows, rows), rows)
    return near, far


def dot(a, b):
    return jnp.dot(a, b, preferred_element_type=f32)


def total(partial):
    return jnp.sum(lane_sums(partial), axis=1, keepdims=True)


def first_half(grad, right, held, grad_sq, ready):
    near, far = sides(grad.shape[0])
    ready(0)
    yours = dot(held[0, :, near], right[...]) + dot(held[0, :, far], held[1])
    squared = squares(held[0])
    held[0] = yours.astype(jnp.bfloat16)
    ready(1)
    mine = dot(grad[:, near], right[...]) + dot(grad[:, far], held[1])
    held[1] = mine.astype(jnp.bfloat16)
    grad_sq[...] = jnp.broadcast_to(total(squared + squares(grad[...])), grad_sq.shape)


def second_half(left, held, grad_sq, ratio, ready):
    near, far = sides(left.shape[0])
    yours = dot(held[2, :, near], held[1]) + dot(held[2, :, far], held[0])
    squared = squares(yours)
    ready()
    mine = dot(left[:, near], held[1]) + dot(left[:, far], held[0])
    squared = squared + squares(mine)
    upper = mine.astype(jnp.bfloat16)
    held[0] = upper
    held[1] = (mine - upper.astype(f32)).astype(jnp.bfloat16)
    entries = BLK * BLK
    ratio[...] = jnp.sqrt(
        (grad_sq[...] / entries + epsilon) / (total(squared) / entries + epsilon)
    )


def middle_kernel(plane, own, heard, sent, held, grad_sq, row, sem):
    row[...] = jnp.broadcast_to(jnp.sum(plane[...], axis=0, keepdims=True), row.shape)
    copy = pltpu.make_async_copy(row, sent, sem)
    copy.start()

    @pl.when(lax.axis_index(LINE) < EARLY_PLANES)
    def _():
        first_half(own.at[0], own.at[1], held, grad_sq, lambda i: None)

    copy.wait()


def late_kernel(grad, right, left, heard, early_sq, held, ratio, own, grad_sq, sems):
    load = pltpu.make_async_copy(left, own.at[2], sems.at[2])
    load.start()
    early = lax.axis_index(LINE) < EARLY_PLANES

    @pl.when(jnp.logical_not(early))
    def _():
        copies = [
            pltpu.make_async_copy(right, own.at[1], sems.at[1]),
            pltpu.make_async_copy(grad, own.at[0], sems.at[0]),
        ]
        for copy in copies:
            copy.start()
        first_half(own.at[0], own.at[1], held, grad_sq, lambda i: copies[i].wait())

    @pl.when(early)
    def _():
        grad_sq[...] = early_sq[...]

    second_half(own.at[2], held, grad_sq, ratio, load.wait)


def middle(plane, own, heard, members):
    return pl.pallas_call(
        middle_kernel,
        out_shape=(
            pltpu.HBM((members, LANES), f32),
            pltpu.VMEM(heard.shape, heard.dtype),
            pltpu.VMEM((8, LANES), f32),
        ),
        in_specs=[VMEM] * 3,
        out_specs=(HBM, VMEM, VMEM),
        input_output_aliases={2: 1},
        scratch_shapes=[pltpu.VMEM((members, LANES), f32), pltpu.SemaphoreType.DMA],
        compiler_params=pltpu.CompilerParams(vmem_limit_bytes=24 << 20),
        cost_estimate=pl.CostEstimate(flops=10**9, bytes_accessed=10**7, transcendentals=0),
        name="middle",
    )(plane, own, heard)


def late(grad, right, left, heard, early_sq):
    return pl.pallas_call(
        late_kernel,
        out_shape=(pltpu.VMEM(heard.shape, heard.dtype), pltpu.VMEM((8, LANES), f32)),
        in_specs=[HBM, HBM, HBM, VMEM, VMEM],
        out_specs=(VMEM, VMEM),
        input_output_aliases={3: 0},
        scratch_shapes=[
            pltpu.VMEM(heard.shape, heard.dtype),
            pltpu.VMEM((8, LANES), f32),
            pltpu.SemaphoreType.DMA((3,)),
        ],
        compiler_params=pltpu.CompilerParams(vmem_limit_bytes=24 << 20),
        cost_estimate=pl.CostEstimate(flops=4 * 10**9, bytes_accessed=10**7, transcendentals=0),
        name="late",
    )(grad, right, left, heard, early_sq)


def final_kernel(count, line, held, ratio, update, staged, sems):
    rows = held.shape[1]
    step = rows // 4
    global_sq = jnp.sum(jnp.sum(line[...], axis=0, keepdims=True), axis=1, keepdims=True)
    scale = clip_rms / jnp.sqrt(global_sq / count + epsilon) * ratio[0:1, 0:1]
    writes = []
    for i in range(4):
        piece = pl.ds(i * step, step)
        result = held[0, piece, :].astype(f32) + held[1, piece, :].astype(f32)
        staged[piece, :] = (scale * result).astype(jnp.bfloat16)
        writes.append(pltpu.make_async_copy(staged.at[piece], update.at[piece], sems.at[i]))
        writes[-1].start()
    for copy in writes:
        copy.wait()


def final(count, line, held, ratio):
    _, rows, columns = held.shape
    return pl.pallas_call(
        functools.partial(final_kernel, count),
        out_shape=jax.ShapeDtypeStruct((rows, columns), jnp.bfloat16),
        in_specs=[VMEM] * 3,
        out_specs=HBM,
        scratch_shapes=[
            pltpu.VMEM((rows, columns), jnp.bfloat16),
            pltpu.SemaphoreType.DMA((4,)),
        ],
        compiler_params=pltpu.CompilerParams(vmem_limit_bytes=16 << 20),
        name="final",
    )(line, held, ratio)


def shards(grad, left_root, right_root):
    plane_size, line_size = lax.axis_size(PLANE), lax.axis_size(LINE)
    count = float(plane_size * line_size // 2 * BLK * BLK)
    grad, left_root, right_root = (in_hbm(x) for x in (grad, left_root, right_root))
    own, sent = head(grad, left_root, right_root, plane_size)
    with jax.named_scope("plane"):
        plane = tell_all(sent, PLANE, PLANE_FIRST)
    with jax.named_scope("exchange"):
        heard = partner(own, PLANE)
    sent, held, early_sq = middle(in_vmem(plane), own, heard, line_size)
    with jax.named_scope("line"):
        line = tell_all(sent, LINE, LINE_FIRST)
    held, ratio = late(grad, right_root, left_root, held, early_sq)
    return final(count, in_vmem(line), held, ratio)


def solution(mesh):
    torus = Mesh(mesh.devices.reshape(16, 32), ALL)
    return jax.shard_map(
        shards,
        mesh=torus,
        in_specs=(P(ALL, None), P(ALL, None), P(ALL, None)),
        out_specs=P(ALL, None),
        check_vma=False,
    )
```

```python
import functools

import jax
import jax.numpy as jnp
from jax import lax
from jax.experimental import pallas as pl
from jax.experimental.pallas import tpu as pltpu
from jax.sharding import Mesh
from jax.sharding import PartitionSpec as P

BLK = 1024
DEV = "dev"
PLANES = 16
SWAPPED_PLANES = (10,)
LINE_FIRST = 10
PLANE_FIRST = 11
EARLY_PLANES = 4
LANES = 128

epsilon = 1e-06
clip_rms = 1.0
f32 = jnp.float32


def partner(shard, axis):
    return lax.ppermute(shard, axis, [(i, i ^ 1) for i in range(lax.axis_size(axis))])


def tell_all(rows, groups):
    return lax.all_to_all(rows, DEV, 0, 0, axis_index_groups=groups, tiled=True)


def plane_groups(planes, across):
    order = [(PLANE_FIRST + i) % across for i in range(across)]
    return [[z * across + i for i in order] for z in range(planes)]


def line_groups(planes, across):
    order = [(LINE_FIRST + z) % planes for z in range(planes)]

    def place(z, i):
        return z * across + (i ^ 1 if z in SWAPPED_PLANES and i > 1 else i)

    return [[place(z, i) for z in order] for i in range(across)]


def in_hbm(array):
    return pltpu.with_memory_space_constraint(array, pltpu.HBM)


def in_vmem(array):
    return pltpu.with_memory_space_constraint(array, pltpu.VMEM)


def squares(values):
    values = values.astype(f32)
    rows, columns = values.shape
    return jnp.sum((values * values).reshape(rows // 8, 8, columns), axis=0)


def lane_sums(partial):
    rows = jnp.sum(partial, axis=0, keepdims=True)
    return sum(rows[:, i : i + LANES] for i in range(0, rows.shape[1], LANES))


def head_kernel(grad, left, right, held, sent, sems):
    rows = grad.shape[0]
    step = rows // 4
    pieces = []
    for i in range(4):
        piece = pl.ds(i * step, step)
        pieces.append(
            pltpu.make_async_copy(grad.at[piece], held.at[0, piece], sems.at[i])
        )
    others = [
        pltpu.make_async_copy(right, held.at[1], sems.at[4]),
        pltpu.make_async_copy(left, held.at[2], sems.at[5]),
    ]
    for copy in pieces + others:
        copy.start()
    total = jnp.zeros((8, grad.shape[1]), f32)
    for i, copy in enumerate(pieces):
        copy.wait()
        total = total + squares(held[0, pl.ds(i * step, step), :])
    sent[...] = jnp.broadcast_to(lane_sums(total), sent.shape)
    for copy in others:
        copy.wait()


VMEM = pl.BlockSpec(memory_space=pltpu.VMEM)
HBM = pl.BlockSpec(memory_space=pltpu.HBM)
ANY = pl.BlockSpec(memory_space=pl.ANY)


def head(grad, left, right, members):
    rows, columns = grad.shape
    return pl.pallas_call(
        head_kernel,
        out_shape=(
            pltpu.VMEM((3, rows, columns), grad.dtype),
            pltpu.VMEM((members, LANES), f32),
        ),
        in_specs=[HBM, HBM, HBM],
        out_specs=(VMEM, VMEM),
        scratch_shapes=[pltpu.SemaphoreType.DMA((6,))],
        cost_estimate=pl.CostEstimate(
            flops=2 * rows * columns, bytes_accessed=6 * rows * columns, transcendentals=0
        ),
        compiler_params=pltpu.CompilerParams(vmem_limit_bytes=16 << 20),
        name="head",
    )(grad, left, right)


def sides(rows):
    parity = lax.axis_index(DEV) % 2
    near = pl.ds(pl.multiple_of(parity * rows, rows), rows)
    far = pl.ds(pl.multiple_of((1 - parity) * rows, rows), rows)
    return near, far


def dot(a, b):
    return jnp.dot(a, b, preferred_element_type=f32)


def total(partial):
    return jnp.sum(lane_sums(partial), axis=1, keepdims=True)


def first_half(grad, right, held, grad_sq, ready):
    near, far = sides(grad.shape[0])
    ready(0)
    yours = dot(held[0, :, near], right[...]) + dot(held[0, :, far], held[1])
    squared = squares(held[0])
    held[0] = yours.astype(jnp.bfloat16)
    ready(1)
    mine = dot(grad[:, near], right[...]) + dot(grad[:, far], held[1])
    held[1] = mine.astype(jnp.bfloat16)
    grad_sq[...] = jnp.broadcast_to(total(squared + squares(grad[...])), grad_sq.shape)


def second_half(left, held, grad_sq, ratio, ready):
    near, far = sides(left.shape[0])
    yours = dot(held[2, :, near], held[1]) + dot(held[2, :, far], held[0])
    squared = squares(yours)
    ready()
    mine = dot(left[:, near], held[1]) + dot(left[:, far], held[0])
    squared = squared + squares(mine)
    upper = mine.astype(jnp.bfloat16)
    held[0] = upper
    held[1] = (mine - upper.astype(f32)).astype(jnp.bfloat16)
    entries = BLK * BLK
    ratio[...] = jnp.sqrt(
        (grad_sq[...] / entries + epsilon) / (total(squared) / entries + epsilon)
    )


def middle_kernel(plane, own, heard, sent, held, grad_sq, row, sem):
    row[...] = jnp.broadcast_to(jnp.sum(plane[...], axis=0, keepdims=True), row.shape)
    copy = pltpu.make_async_copy(row, sent, sem)
    copy.start()

    @pl.when(lax.axis_index(DEV) < EARLY_PLANES * (lax.axis_size(DEV) // PLANES))
    def _():
        first_half(own.at[0], own.at[1], held, grad_sq, lambda i: None)

    copy.wait()


def late_kernel(grad, right, left, heard, early_sq, held, ratio, own, grad_sq, sems):
    load = pltpu.make_async_copy(left, own.at[2], sems.at[2])
    load.start()
    early = lax.axis_index(DEV) < EARLY_PLANES * (lax.axis_size(DEV) // PLANES)

    @pl.when(jnp.logical_not(early))
    def _():
        copies = [
            pltpu.make_async_copy(right, own.at[1], sems.at[1]),
            pltpu.make_async_copy(grad, own.at[0], sems.at[0]),
        ]
        for copy in copies:
            copy.start()
        first_half(own.at[0], own.at[1], held, grad_sq, lambda i: copies[i].wait())

    @pl.when(early)
    def _():
        grad_sq[...] = early_sq[...]

    second_half(own.at[2], held, grad_sq, ratio, load.wait)


def middle(plane, own, heard, members):
    return pl.pallas_call(
        middle_kernel,
        out_shape=(
            pltpu.HBM((members, LANES), f32),
            pltpu.VMEM(heard.shape, heard.dtype),
            pltpu.VMEM((8, LANES), f32),
        ),
        in_specs=[VMEM] * 3,
        out_specs=(HBM, VMEM, VMEM),
        input_output_aliases={2: 1},
        scratch_shapes=[pltpu.VMEM((members, LANES), f32), pltpu.SemaphoreType.DMA],
        compiler_params=pltpu.CompilerParams(vmem_limit_bytes=24 << 20),
        cost_estimate=pl.CostEstimate(flops=10**9, bytes_accessed=10**7, transcendentals=0),
        name="middle",
    )(plane, own, heard)


def late(grad, right, left, heard, early_sq):
    return pl.pallas_call(
        late_kernel,
        out_shape=(pltpu.VMEM(heard.shape, heard.dtype), pltpu.VMEM((8, LANES), f32)),
        in_specs=[HBM, HBM, HBM, VMEM, VMEM],
        out_specs=(VMEM, VMEM),
        input_output_aliases={3: 0},
        scratch_shapes=[
            pltpu.VMEM(heard.shape, heard.dtype),
            pltpu.VMEM((8, LANES), f32),
            pltpu.SemaphoreType.DMA((3,)),
        ],
        compiler_params=pltpu.CompilerParams(vmem_limit_bytes=24 << 20),
        cost_estimate=pl.CostEstimate(flops=4 * 10**9, bytes_accessed=10**7, transcendentals=0),
        name="late",
    )(grad, right, left, heard, early_sq)


def final_kernel(count, line, held, ratio, update, staged, sems):
    rows = held.shape[1]
    step = rows // 8
    global_sq = jnp.sum(jnp.sum(line[...], axis=0, keepdims=True), axis=1, keepdims=True)
    scale = clip_rms / jnp.sqrt(global_sq / count + epsilon) * ratio[0:1, 0:1]
    writes = []
    for i in range(8):
        piece = pl.ds(i * step, step)
        result = held[0, piece, :].astype(f32) + held[1, piece, :].astype(f32)
        staged[piece, :] = (scale * result).astype(jnp.bfloat16)
        writes.append(pltpu.make_async_copy(staged.at[piece], update.at[piece], sems.at[i]))
        writes[-1].start()
    for copy in writes:
        copy.wait()


def final(count, line, held, ratio):
    _, rows, columns = held.shape
    return pl.pallas_call(
        functools.partial(final_kernel, count),
        out_shape=jax.ShapeDtypeStruct((rows, columns), jnp.bfloat16),
        in_specs=[VMEM] * 3,
        out_specs=HBM,
        scratch_shapes=[
            pltpu.VMEM((rows, columns), jnp.bfloat16),
            pltpu.SemaphoreType.DMA((8,)),
        ],
        compiler_params=pltpu.CompilerParams(vmem_limit_bytes=16 << 20),
        name="final",
    )(line, held, ratio)


def shards(grad, left_root, right_root):
    plane_size, line_size = lax.axis_size(DEV) // PLANES, PLANES
    count = float(plane_size * line_size // 2 * BLK * BLK)
    grad, left_root, right_root = (in_hbm(x) for x in (grad, left_root, right_root))
    own, sent = head(grad, left_root, right_root, plane_size)
    with jax.named_scope("plane"):
        plane = tell_all(sent, plane_groups(line_size, plane_size))
    with jax.named_scope("exchange"):
        heard = partner(own, DEV)
    sent, held, early_sq = middle(in_vmem(plane), own, heard, line_size)
    with jax.named_scope("line"):
        line = tell_all(sent, line_groups(line_size, plane_size))
    held, ratio = late(grad, right_root, left_root, held, early_sq)
    return final(count, in_vmem(line), held, ratio)


def solution(mesh):
    torus = Mesh(mesh.devices.reshape(mesh.size), (DEV,))
    return jax.shard_map(
        shards,
        mesh=torus,
        in_specs=(P(DEV, None), P(DEV, None), P(DEV, None)),
        out_specs=P(DEV, None),
        check_vma=False,
    )
```

```python
import functools

import jax
import jax.numpy as jnp
from jax import lax
from jax.experimental import pallas as pl
from jax.experimental.pallas import tpu as pltpu
from jax.sharding import Mesh
from jax.sharding import PartitionSpec as P

BLK = 1024
DEV = "dev"
PLANES = 16
SWAPPED_PLANES = (11, 15)
LINE_FIRST = 11
PLANE_FIRST = 11
EARLY_PLANES = 4
LANES = 128

epsilon = 1e-06
clip_rms = 1.0
f32 = jnp.float32


def partner(shard, axis):
    return lax.ppermute(shard, axis, [(i, i ^ 1) for i in range(lax.axis_size(axis))])


def tell_all(rows, groups):
    return lax.all_to_all(rows, DEV, 0, 0, axis_index_groups=groups, tiled=True)


def plane_groups(planes, across):
    order = [(PLANE_FIRST + i) % across for i in range(across)]
    return [[z * across + i for i in order] for z in range(planes)]


def line_groups(planes, across):
    order = [(LINE_FIRST + z) % planes for z in range(planes)]

    def place(z, i):
        return z * across + (i ^ 1 if z in SWAPPED_PLANES and i > 1 else i)

    return [[place(z, i) for z in order] for i in range(across)]


def in_hbm(array):
    return pltpu.with_memory_space_constraint(array, pltpu.HBM)


def in_vmem(array):
    return pltpu.with_memory_space_constraint(array, pltpu.VMEM)


def squares(values):
    values = values.astype(f32)
    rows, columns = values.shape
    return jnp.sum((values * values).reshape(rows // 8, 8, columns), axis=0)


def lane_sums(partial):
    rows = jnp.sum(partial, axis=0, keepdims=True)
    return sum(rows[:, i : i + LANES] for i in range(0, rows.shape[1], LANES))


def head_kernel(grad, left, right, held, sent, sems):
    rows = grad.shape[0]
    step = rows // 4
    pieces = []
    for i in range(4):
        piece = pl.ds(i * step, step)
        pieces.append(
            pltpu.make_async_copy(grad.at[piece], held.at[0, piece], sems.at[i])
        )
    others = [
        pltpu.make_async_copy(right, held.at[1], sems.at[4]),
        pltpu.make_async_copy(left, held.at[2], sems.at[5]),
    ]
    for copy in pieces + others:
        copy.start()
    total = jnp.zeros((8, grad.shape[1]), f32)
    for i, copy in enumerate(pieces):
        copy.wait()
        total = total + squares(held[0, pl.ds(i * step, step), :])
    sent[...] = jnp.broadcast_to(lane_sums(total), sent.shape)
    for copy in others:
        copy.wait()


VMEM = pl.BlockSpec(memory_space=pltpu.VMEM)
HBM = pl.BlockSpec(memory_space=pltpu.HBM)
ANY = pl.BlockSpec(memory_space=pl.ANY)


def head(grad, left, right, members):
    rows, columns = grad.shape
    return pl.pallas_call(
        head_kernel,
        out_shape=(
            pltpu.VMEM((3, rows, columns), grad.dtype),
            pltpu.VMEM((members, LANES), f32),
        ),
        in_specs=[HBM, HBM, HBM],
        out_specs=(VMEM, VMEM),
        scratch_shapes=[pltpu.SemaphoreType.DMA((6,))],
        cost_estimate=pl.CostEstimate(
            flops=2 * rows * columns, bytes_accessed=6 * rows * columns, transcendentals=0
        ),
        compiler_params=pltpu.CompilerParams(vmem_limit_bytes=16 << 20),
        name="head",
    )(grad, left, right)


def sides(rows):
    parity = lax.axis_index(DEV) % 2
    near = pl.ds(pl.multiple_of(parity * rows, rows), rows)
    far = pl.ds(pl.multiple_of((1 - parity) * rows, rows), rows)
    return near, far


def dot(a, b):
    return jnp.dot(a, b, preferred_element_type=f32)


def total(partial):
    return jnp.sum(lane_sums(partial), axis=1, keepdims=True)


def first_half(grad, right, held, grad_sq, ready):
    near, far = sides(grad.shape[0])
    ready(0)
    yours = dot(held[0, :, near], right[...]) + dot(held[0, :, far], held[1])
    squared = squares(held[0])
    held[0] = yours.astype(jnp.bfloat16)
    ready(1)
    mine = dot(grad[:, near], right[...]) + dot(grad[:, far], held[1])
    held[1] = mine.astype(jnp.bfloat16)
    grad_sq[...] = jnp.broadcast_to(total(squared + squares(grad[...])), grad_sq.shape)


def second_half(left, held, grad_sq, ratio, ready):
    near, far = sides(left.shape[0])
    yours = dot(held[2, :, near], held[1]) + dot(held[2, :, far], held[0])
    squared = squares(yours)
    ready()
    mine = dot(left[:, near], held[1]) + dot(left[:, far], held[0])
    squared = squared + squares(mine)
    upper = mine.astype(jnp.bfloat16)
    held[0] = upper
    held[1] = (mine - upper.astype(f32)).astype(jnp.bfloat16)
    entries = BLK * BLK
    ratio[...] = jnp.sqrt(
        (grad_sq[...] / entries + epsilon) / (total(squared) / entries + epsilon)
    )


def middle_kernel(plane, own, heard, sent, held, grad_sq, row, sem):
    row[...] = jnp.broadcast_to(jnp.sum(plane[...], axis=0, keepdims=True), row.shape)
    copy = pltpu.make_async_copy(row, sent, sem)
    copy.start()

    @pl.when(lax.axis_index(DEV) < EARLY_PLANES * (lax.axis_size(DEV) // PLANES))
    def _():
        first_half(own.at[0], own.at[1], held, grad_sq, lambda i: None)

    copy.wait()


def late_kernel(grad, right, left, heard, early_sq, held, ratio, own, grad_sq, sems):
    load = pltpu.make_async_copy(left, own.at[2], sems.at[2])
    load.start()
    early = lax.axis_index(DEV) < EARLY_PLANES * (lax.axis_size(DEV) // PLANES)

    @pl.when(jnp.logical_not(early))
    def _():
        copies = [
            pltpu.make_async_copy(right, own.at[1], sems.at[1]),
            pltpu.make_async_copy(grad, own.at[0], sems.at[0]),
        ]
        for copy in copies:
            copy.start()
        first_half(own.at[0], own.at[1], held, grad_sq, lambda i: copies[i].wait())

    @pl.when(early)
    def _():
        grad_sq[...] = early_sq[...]

    second_half(own.at[2], held, grad_sq, ratio, load.wait)


def middle(plane, own, heard, members):
    return pl.pallas_call(
        middle_kernel,
        out_shape=(
            pltpu.HBM((members, LANES), f32),
            pltpu.VMEM(heard.shape, heard.dtype),
            pltpu.VMEM((8, LANES), f32),
        ),
        in_specs=[VMEM] * 3,
        out_specs=(HBM, VMEM, VMEM),
        input_output_aliases={2: 1},
        scratch_shapes=[pltpu.VMEM((members, LANES), f32), pltpu.SemaphoreType.DMA],
        compiler_params=pltpu.CompilerParams(vmem_limit_bytes=24 << 20),
        cost_estimate=pl.CostEstimate(flops=10**9, bytes_accessed=10**7, transcendentals=0),
        name="middle",
    )(plane, own, heard)


def late(grad, right, left, heard, early_sq):
    return pl.pallas_call(
        late_kernel,
        out_shape=(pltpu.VMEM(heard.shape, heard.dtype), pltpu.VMEM((8, LANES), f32)),
        in_specs=[HBM, HBM, HBM, VMEM, VMEM],
        out_specs=(VMEM, VMEM),
        input_output_aliases={3: 0},
        scratch_shapes=[
            pltpu.VMEM(heard.shape, heard.dtype),
            pltpu.VMEM((8, LANES), f32),
            pltpu.SemaphoreType.DMA((3,)),
        ],
        compiler_params=pltpu.CompilerParams(vmem_limit_bytes=24 << 20),
        cost_estimate=pl.CostEstimate(flops=4 * 10**9, bytes_accessed=10**7, transcendentals=0),
        name="late",
    )(grad, right, left, heard, early_sq)


def final_kernel(count, line, held, ratio, update, staged, sems):
    rows = held.shape[1]
    step = rows // 8
    global_sq = jnp.sum(jnp.sum(line[...], axis=0, keepdims=True), axis=1, keepdims=True)
    scale = clip_rms / jnp.sqrt(global_sq / count + epsilon) * ratio[0:1, 0:1]
    writes = []
    for i in range(8):
        piece = pl.ds(i * step, step)
        result = held[0, piece, :].astype(f32) + held[1, piece, :].astype(f32)
        staged[piece, :] = (scale * result).astype(jnp.bfloat16)
        writes.append(pltpu.make_async_copy(staged.at[piece], update.at[piece], sems.at[i]))
        writes[-1].start()
    for copy in writes:
        copy.wait()


def final(count, line, held, ratio):
    _, rows, columns = held.shape
    return pl.pallas_call(
        functools.partial(final_kernel, count),
        out_shape=jax.ShapeDtypeStruct((rows, columns), jnp.bfloat16),
        in_specs=[VMEM] * 3,
        out_specs=HBM,
        scratch_shapes=[
            pltpu.VMEM((rows, columns), jnp.bfloat16),
            pltpu.SemaphoreType.DMA((8,)),
        ],
        compiler_params=pltpu.CompilerParams(vmem_limit_bytes=16 << 20),
        name="final",
    )(line, held, ratio)


def shards(grad, left_root, right_root):
    plane_size, line_size = lax.axis_size(DEV) // PLANES, PLANES
    count = float(plane_size * line_size // 2 * BLK * BLK)
    grad, left_root, right_root = (in_hbm(x) for x in (grad, left_root, right_root))
    own, sent = head(grad, left_root, right_root, plane_size)
    with jax.named_scope("plane"):
        plane = tell_all(sent, plane_groups(line_size, plane_size))
    with jax.named_scope("exchange"):
        heard = partner(own, DEV)
    sent, held, early_sq = middle(in_vmem(plane), own, heard, line_size)
    with jax.named_scope("line"):
        line = tell_all(sent, line_groups(line_size, plane_size))
    held, ratio = late(grad, right_root, left_root, held, early_sq)
    return final(count, in_vmem(line), held, ratio)


def solution(mesh):
    torus = Mesh(mesh.devices.reshape(mesh.size), (DEV,))
    return jax.shard_map(
        shards,
        mesh=torus,
        in_specs=(P(DEV, None), P(DEV, None), P(DEV, None)),
        out_specs=P(DEV, None),
        check_vma=False,
    )
```

```python
import functools

import jax
import jax.numpy as jnp
from jax import lax
from jax.experimental import pallas as pl
from jax.experimental.pallas import tpu as pltpu
from jax.sharding import Mesh
from jax.sharding import PartitionSpec as P

BLK = 1024
DEV = "dev"
PLANES = 16
SWAPPED_PLANES = (11, 15)
LINE_FIRST = 11
PLANE_FIRST = 11
EARLY_PLANES = 4
LANES = 128

epsilon = 1e-06
clip_rms = 1.0
f32 = jnp.float32


def partner(shard, axis):
    return lax.ppermute(shard, axis, [(i, i ^ 1) for i in range(lax.axis_size(axis))])


def tell_all(rows, groups):
    return lax.all_to_all(rows, DEV, 0, 0, axis_index_groups=groups, tiled=True)


def plane_groups(planes, across):
    order = [(PLANE_FIRST + i) % across for i in range(across)]
    return [[z * across + i for i in order] for z in range(planes)]


def line_groups(planes, across):
    order = [(LINE_FIRST + z) % planes for z in range(planes)]

    def place(z, i):
        return z * across + (i ^ 1 if z in SWAPPED_PLANES and i > 1 else i)

    return [[place(z, i) for z in order] for i in range(across)]


def in_hbm(array):
    return pltpu.with_memory_space_constraint(array, pltpu.HBM)


def in_vmem(array):
    return pltpu.with_memory_space_constraint(array, pltpu.VMEM)


def squares(values):
    values = values.astype(f32)
    rows, columns = values.shape
    return jnp.sum((values * values).reshape(rows // 8, 8, columns), axis=0)


def lane_sums(partial):
    rows = jnp.sum(partial, axis=0, keepdims=True)
    return sum(rows[:, i : i + LANES] for i in range(0, rows.shape[1], LANES))


def head_kernel(grad, left, right, held, sent, sems):
    rows = grad.shape[0]
    step = rows // 4
    pieces = []
    for i in range(4):
        piece = pl.ds(i * step, step)
        pieces.append(
            pltpu.make_async_copy(grad.at[piece], held.at[0, piece], sems.at[i])
        )
    others = [
        pltpu.make_async_copy(right, held.at[1], sems.at[4]),
        pltpu.make_async_copy(left, held.at[2], sems.at[5]),
    ]
    for copy in pieces + others:
        copy.start()
    total = jnp.zeros((8, grad.shape[1]), f32)
    for i, copy in enumerate(pieces):
        copy.wait()
        total = total + squares(held[0, pl.ds(i * step, step), :])
    sent[...] = jnp.broadcast_to(lane_sums(total), sent.shape)
    for copy in others:
        copy.wait()


VMEM = pl.BlockSpec(memory_space=pltpu.VMEM)
HBM = pl.BlockSpec(memory_space=pltpu.HBM)
ANY = pl.BlockSpec(memory_space=pl.ANY)


def head(grad, left, right, members):
    rows, columns = grad.shape
    return pl.pallas_call(
        head_kernel,
        out_shape=(
            pltpu.VMEM((3, rows, columns), grad.dtype),
            pltpu.VMEM((members, LANES), f32),
        ),
        in_specs=[HBM, HBM, HBM],
        out_specs=(VMEM, VMEM),
        scratch_shapes=[pltpu.SemaphoreType.DMA((6,))],
        cost_estimate=pl.CostEstimate(
            flops=2 * rows * columns, bytes_accessed=6 * rows * columns, transcendentals=0
        ),
        compiler_params=pltpu.CompilerParams(vmem_limit_bytes=16 << 20),
        name="head",
    )(grad, left, right)


def sides(rows):
    parity = lax.axis_index(DEV) % 2
    near = pl.ds(pl.multiple_of(parity * rows, rows), rows)
    far = pl.ds(pl.multiple_of((1 - parity) * rows, rows), rows)
    return near, far


def dot(a, b):
    return jnp.dot(a, b, preferred_element_type=f32)


def total(partial):
    return jnp.sum(lane_sums(partial), axis=1, keepdims=True)


def first_half(grad, right, held, grad_sq, ready):
    near, far = sides(grad.shape[0])
    ready(0)
    yours = dot(held[0, :, near], right[...]) + dot(held[0, :, far], held[1])
    squared = squares(held[0])
    held[0] = yours.astype(jnp.bfloat16)
    ready(1)
    mine = dot(grad[:, near], right[...]) + dot(grad[:, far], held[1])
    held[1] = mine.astype(jnp.bfloat16)
    grad_sq[...] = jnp.broadcast_to(total(squared + squares(grad[...])), grad_sq.shape)


def second_half(left, held, grad_sq, ratio, ready):
    near, far = sides(left.shape[0])
    yours = dot(held[2, :, near], held[1]) + dot(held[2, :, far], held[0])
    squared = squares(yours)
    ready()
    mine = dot(left[:, near], held[1]) + dot(left[:, far], held[0])
    squared = squared + squares(mine)
    upper = mine.astype(jnp.bfloat16)
    held[0] = upper
    held[1] = (mine - upper.astype(f32)).astype(jnp.bfloat16)
    entries = BLK * BLK
    ratio[...] = jnp.sqrt(
        (grad_sq[...] / entries + epsilon) / (total(squared) / entries + epsilon)
    )


def middle_kernel(plane, own, heard, sent, held, grad_sq, row, sem):
    row[...] = jnp.broadcast_to(jnp.sum(plane[...], axis=0, keepdims=True), row.shape)
    copy = pltpu.make_async_copy(row, sent, sem)
    copy.start()

    @pl.when(lax.axis_index(DEV) < EARLY_PLANES * (lax.axis_size(DEV) // PLANES))
    def _():
        first_half(own.at[0], own.at[1], held, grad_sq, lambda i: None)

    copy.wait()


def late_kernel(grad, right, left, heard, early_sq, held, ratio, own, grad_sq, sems):
    load = pltpu.make_async_copy(left, own.at[2], sems.at[2])
    load.start()
    early = lax.axis_index(DEV) < EARLY_PLANES * (lax.axis_size(DEV) // PLANES)

    @pl.when(jnp.logical_not(early))
    def _():
        copies = [
            pltpu.make_async_copy(right, own.at[1], sems.at[1]),
            pltpu.make_async_copy(grad, own.at[0], sems.at[0]),
        ]
        for copy in copies:
            copy.start()
        first_half(own.at[0], own.at[1], held, grad_sq, lambda i: copies[i].wait())

    @pl.when(early)
    def _():
        grad_sq[...] = early_sq[...]

    second_half(own.at[2], held, grad_sq, ratio, load.wait)


def middle(plane, own, heard, members):
    return pl.pallas_call(
        middle_kernel,
        out_shape=(
            pltpu.HBM((members, LANES), f32),
            pltpu.VMEM(heard.shape, heard.dtype),
            pltpu.VMEM((8, LANES), f32),
        ),
        in_specs=[VMEM] * 3,
        out_specs=(HBM, VMEM, VMEM),
        input_output_aliases={2: 1},
        scratch_shapes=[pltpu.VMEM((members, LANES), f32), pltpu.SemaphoreType.DMA],
        compiler_params=pltpu.CompilerParams(vmem_limit_bytes=24 << 20),
        cost_estimate=pl.CostEstimate(flops=10**9, bytes_accessed=10**7, transcendentals=0),
        name="middle",
    )(plane, own, heard)


def late(grad, right, left, heard, early_sq):
    return pl.pallas_call(
        late_kernel,
        out_shape=(pltpu.VMEM(heard.shape, heard.dtype), pltpu.VMEM((8, LANES), f32)),
        in_specs=[HBM, HBM, HBM, VMEM, VMEM],
        out_specs=(VMEM, VMEM),
        input_output_aliases={3: 0},
        scratch_shapes=[
            pltpu.VMEM(heard.shape, heard.dtype),
            pltpu.VMEM((8, LANES), f32),
            pltpu.SemaphoreType.DMA((3,)),
        ],
        compiler_params=pltpu.CompilerParams(vmem_limit_bytes=24 << 20),
        cost_estimate=pl.CostEstimate(flops=4 * 10**9, bytes_accessed=10**7, transcendentals=0),
        name="late",
    )(grad, right, left, heard, early_sq)


def final_kernel(count, line, held, ratio, update, staged, sems):
    rows = held.shape[1]
    global_sq = jnp.sum(jnp.sum(line[...], axis=0, keepdims=True), axis=1, keepdims=True)
    scale = clip_rms * lax.rsqrt(global_sq / count + epsilon) * ratio[0:1, 0:1]
    writes = []
    edges = [0, 1, 2, 4, 6, 8, 10, 12, 14, 15, 16]
    for i, (start, stop) in enumerate(zip(edges, edges[1:])):
        piece = pl.ds(start * rows // 16, (stop - start) * rows // 16)
        result = held[0, piece, :].astype(f32) + held[1, piece, :].astype(f32)
        staged[piece, :] = (scale * result).astype(jnp.bfloat16)
        writes.append(pltpu.make_async_copy(staged.at[piece], update.at[piece], sems.at[i]))
        writes[-1].start()
    for copy in writes:
        copy.wait()


def final(count, line, held, ratio):
    _, rows, columns = held.shape
    return pl.pallas_call(
        functools.partial(final_kernel, count),
        out_shape=jax.ShapeDtypeStruct((rows, columns), jnp.bfloat16),
        in_specs=[VMEM] * 3,
        out_specs=HBM,
        scratch_shapes=[
            pltpu.VMEM((rows, columns), jnp.bfloat16),
            pltpu.SemaphoreType.DMA((10,)),
        ],
        compiler_params=pltpu.CompilerParams(vmem_limit_bytes=16 << 20),
        name="final",
    )(line, held, ratio)


def shards(grad, left_root, right_root):
    plane_size, line_size = lax.axis_size(DEV) // PLANES, PLANES
    count = float(plane_size * line_size // 2 * BLK * BLK)
    grad, left_root, right_root = (in_hbm(x) for x in (grad, left_root, right_root))
    own, sent = head(grad, left_root, right_root, plane_size)
    with jax.named_scope("plane"):
        plane = tell_all(sent, plane_groups(line_size, plane_size))
    with jax.named_scope("exchange"):
        heard = partner(own, DEV)
    sent, held, early_sq = middle(in_vmem(plane), own, heard, line_size)
    with jax.named_scope("line"):
        line = tell_all(sent, line_groups(line_size, plane_size))
    held, ratio = late(grad, right_root, left_root, held, early_sq)
    return final(count, in_vmem(line), held, ratio)


def solution(mesh):
    torus = Mesh(mesh.devices.reshape(mesh.size), (DEV,))
    return jax.shard_map(
        shards,
        mesh=torus,
        in_specs=(P(DEV, None), P(DEV, None), P(DEV, None)),
        out_specs=P(DEV, None),
        check_vma=False,
    )
```
